256 devices in a mesh: dp: 64 (over z, x, y_lo), mp: 4 (over y_hi, core).
Axes of the slice: x: 4, y: 4 (y_hi: 2, y_lo: 2; y = y_hi * 2 + y_lo), z: 8, core: 2. Of those that a mesh axis runs over, the one named last changes fastest.
Arguments:
- patches: bfloat16 [32768, 2048], P('dp'), may hold values from -16 to 16
- cotangent: bfloat16 [32768, 8192], P('dp', 'mp'), may hold values from -0.03125 to 0.03125
- weight: float32 [2048, 8192], P('dp', 'mp'), may hold values from -0.125 to 0.125
- accum: float32 [2048, 8192], P('dp', 'mp'), may hold values from 0.1 to 4
Outputs:
- new_weight: float32 [2048, 8192], P(('dp', 'mp'))
- new_accum: float32 [2048, 8192], P(('dp', 'mp'))
- weight_copy: bfloat16 [2048, 8192], P(None, 'mp')
The draws below stay inside these ranges and needn't reach their ends.
All inputs are finite; a program needn't handle non-finite values.
Results may differ from the reference program's by a relative error of at most 0.001.
Values may be sent and summed in bfloat16 or wider, within the bound.
No kernel may reach another device: no remote copies, remote signals or barrier semaphores. Data moves between devices by JAX's collectives and lax.ppermute only.
A program may use at most 192 MiB of HBM per device.

```python
import math
import jax
import jax.numpy as jnp
from jax import lax

D = 2048
FF = 8192
TOKENS = 32768


def spiked(entries, rng, source, target, blocks, factor):
    def block_of(position):
        return (jnp.arange(entries.shape[position]) // (entries.shape[position] // blocks)).reshape((-1,) + (1,) * (entries.ndim - 1 - position))

    one_side = jax.random.permutation(rng, blocks)[block_of(target)]
    far = (block_of(target) + blocks // 2) % blocks
    return jnp.where((block_of(source) == one_side) | (block_of(source) == far), factor * entries, entries)


def block_levels(rng, dims, shards, low, largest):
    def one(position, parts):
        heights = jax.random.uniform(jax.random.fold_in(jax.random.fold_in(rng, 6), position), (parts,), jnp.float32, low / len(shards), largest / len(shards))
        return jnp.repeat(jnp.exp(heights), dims[position] // parts).reshape((-1,) + (1,) * (len(dims) - position - 1))

    loudness = one(*shards[0])
    for cut in shards[1:]:
        loudness = loudness * one(*cut)
    return loudness


def noise(stream_key, shape, width, bound, shards=(), held_as=jnp.bfloat16):
    result = jax.random.normal(stream_key, shape, jnp.float32) * width
    if len(shards) > 0:
        result = block_levels(stream_key, shape, shards, -0.22, 0.18) * result
    return jnp.clip(result, min=-bound, max=bound).astype(held_as)


def noise_with(rng, extent, spread, bound, pieces, heavy, held_as=jnp.bfloat16):
    values = spread * jax.random.normal(rng, extent, jnp.float32)
    if pieces:
        values = values * block_levels(rng, extent, pieces, -0.22, 0.18)
    return jnp.clip(spiked(values, jax.random.fold_in(rng, 3), *heavy), -bound, bound).astype(held_as)


def setup_inputs(seed: int = 0) -> dict:
    key_of = jax.random.split(jax.random.key(seed), 5)
    return {
        "patches": noise_with(key_of[0], (TOKENS, D), 1.0, 16.0, ((0, 64),), (0, 1, 64, 4.0)),
        "cotangent": noise(key_of[1], (TOKENS, FF), TOKENS ** -0.5, 0.03125, ((0, 64), (1, 4))),
        "weight": noise(key_of[2], (D, FF), D ** -0.5, 0.125, ((0, 64), (1, 4)), jnp.float32),
        "accum": jnp.clip(jnp.exp(math.log(4.0) - 3.6888794 * jax.random.uniform(key_of[3], (D, FF), jnp.float32) ** block_levels(key_of[3], (D, FF), ((0, 64), (1, 4)), -0.2, 0.2)), 0.1, 4.0),
    }


learning_rate = 0.02

def reference(patches, cotangent, weight, accum):
    grad = jnp.dot(patches.T, cotangent, preferred_element_type=jnp.float32)
    new_accum = accum + grad * grad
    new_weight = weight - learning_rate * grad * lax.rsqrt(new_accum)
    weight_copy = new_weight.astype(jnp.bfloat16)
    return (new_weight, new_accum, weight_copy)
```

```python
import jax
import jax.numpy as jnp
from jax import lax
from jax.sharding import Mesh
from jax.sharding import PartitionSpec as P

DP = ("dp_0", "dp_1", "dp_2")
DP_MP = ("dp_0", "dp_1", "dp_2", "mp")


learning_rate = 0.02


def adagrad(accum, weight, grad):
    summed = accum + grad * grad
    return (summed, weight - learning_rate * grad * lax.rsqrt(summed))


def shards(patches, cotangent, weight, accum):
    partial = jnp.einsum("tr,tf->rf", patches, cotangent, preferred_element_type=jnp.float32)
    over_zx = lax.psum_scatter(partial, DP[:2], scatter_dimension=0, tiled=True)
    grad_block = lax.psum_scatter(over_zx, DP[2], scatter_dimension=0, tiled=True)
    accum_block, weight_block = adagrad(accum, weight, grad_block)
    pair = lax.all_gather(weight_block.astype(jnp.bfloat16), DP[2], axis=0, tiled=True)
    weight_copy = lax.all_gather(pair, DP[:2], axis=0, tiled=True)
    new_accum, new_weight = (
        lax.all_to_all(accum_block, "mp", split_axis=0, concat_axis=1, tiled=True),
        lax.all_to_all(weight_block, "mp", split_axis=0, concat_axis=1, tiled=True),
    )
    return (new_weight, new_accum, weight_copy)


def solution(mesh):
    finer = Mesh(mesh.devices.reshape(8, 4, 2, mesh.shape["mp"]), ("dp_0", "dp_1", "dp_2", "mp"))
    placed = (P(DP, None), P(DP, "mp"), P(DP, "mp"), P(DP, "mp"))
    return jax.shard_map(
        shards,
        mesh=finer,
        in_specs=placed,
        out_specs=(P(DP_MP, None), P(DP_MP, None), P(None, "mp")),
        check_vma=False,
    )
```

```python
import jax
import jax.numpy as jnp
from jax import lax
from jax.sharding import Mesh
from jax.sharding import PartitionSpec as P

AXES = ("z", "x", "y", "mp")
SIZE = {"z": 8, "x": 4, "y": 2, "mp": 4}
DP = ("z", "x", "y")
SPLIT = 1024

learning_rate = 0.02


def shift(value, axis, by):
    n = SIZE[axis]
    return lax.ppermute(value, axis, [(i, (i + by) % n) for i in range(n)])


def pack(value, summed):
    return (value * (128.0 / summed)).astype(jnp.float16)


def unpack(value, summed):
    return value.astype(jnp.float32) * (summed / 128.0)


def ring_sum(own, axis, per_device):
    n = SIZE[axis]
    half = n // 2
    far = own(half)
    cut = far.shape[-1] // 2
    up = shift(pack(far[..., :cut], half * per_device), axis, 1)
    down = shift(pack(far[..., cut:], half * per_device), axis, -1)
    for step in range(half - 1, 0, -1):
        a, b = own(step), own(n - step)
        got_a, got_b = unpack(up, half * per_device), unpack(down, half * per_device)
        if step == half - 1:
            a = jnp.concatenate([a[..., :cut] + got_a, a[..., cut:]], -1)
            b = jnp.concatenate([b[..., :cut], b[..., cut:] + got_b], -1)
        else:
            a, b = a + got_a, b + got_b
        up = shift(pack(a, half * per_device), axis, 1)
        down = shift(pack(b, half * per_device), axis, -1)
    return own(0) + unpack(up, half * per_device) + unpack(down, half * per_device)


def direct_sum(own, axis, per_device):
    n = SIZE[axis]
    got = [shift(pack(own(k), per_device), axis, k) for k in range(1, n)]
    total = own(0)
    for value in got:
        total = total + unpack(value, per_device)
    return total


def place(out, value, start):
    return lax.dynamic_update_slice(out, value, start)


def shards(patches, cotangent, weight, accum):
    z, x, y = (lax.axis_index(a) for a in DP)
    left, right = cotangent[:, :SPLIT], cotangent[:, SPLIT:]

    def dot(p, c):
        return jnp.einsum("tr,tf->rf", p, c, preferred_element_type=jnp.float32)

    def for_z(k):
        rows = lax.dynamic_slice_in_dim(patches, (z + k) % 8 * 256, 256, 1)
        return dot(rows, left)

    whole = dot(patches, right).reshape(8, 4, 64, -1)

    def for_x(k):
        return lax.dynamic_index_in_dim(whole, (x + k) % 4, 1, False)

    over_x = ring_sum(for_x, "x", 1)
    over_z = ring_sum(for_z, "z", 1)
    right_zx = ring_sum(lambda k: lax.dynamic_index_in_dim(over_x, (z + k) % 8, 0, False), "z", 4)
    left_zx = direct_sum(lambda k: lax.dynamic_slice_in_dim(over_z, (x + k) % 4 * 64, 64, 0), "x", 8)
    both = jnp.concatenate([left_zx, right_zx], -1)
    grad = direct_sum(lambda k: lax.dynamic_slice_in_dim(both, (y + k) % 2 * 32, 32, 0), "y", 32)

    summed = accum + grad * grad
    updated = weight - learning_rate * grad * lax.rsqrt(summed)

    mine = updated.astype(jnp.bfloat16)
    other = shift(mine, "y", 1)
    pair = jnp.where(y == 0, jnp.concatenate([mine, other]), jnp.concatenate([other, mine]))
    copy = jnp.zeros((8, 4, 64, 2048), jnp.bfloat16)

    block = pair[:, SPLIT:]
    blocks = jnp.zeros((8, 64, 2048 - SPLIT), jnp.bfloat16)
    for k, v in gather_ring(block, "z"):
        blocks = place(blocks, v[None], ((z + k) % 8, 0, 0))
    for k, v in gather_ring(blocks, "x"):
        copy = place(copy, v[:, None], (0, (x + k) % 4, 0, SPLIT))
    block = pair[:, :SPLIT]
    blocks = jnp.zeros((4, 64, SPLIT), jnp.bfloat16)
    blocks = place(blocks, block[None], (x, 0, 0))
    for k in range(1, 4):
        blocks = place(blocks, shift(block, "x", -k)[None], ((x + k) % 4, 0, 0))
    for k, v in gather_ring(blocks, "z"):
        copy = place(copy, v[None], ((z + k) % 8, 0, 0, 0))
    weight_copy = copy.reshape(2048, 2048)

    new_accum, new_weight = (
        lax.all_to_all(summed, "mp", split_axis=0, concat_axis=1, tiled=True),
        lax.all_to_all(updated, "mp", split_axis=0, concat_axis=1, tiled=True),
    )
    return (new_weight, new_accum, weight_copy)


def gather_ring(block, axis):
    n = SIZE[axis]
    half = n // 2
    yield 0, block
    up, down = block, block
    for step in range(1, half):
        up, down = shift(up, axis, 1), shift(down, axis, -1)
        yield n - step, up
        yield step, down
    cut = block.shape[-1] // 2
    far = jnp.concatenate([shift(up[..., :cut], axis, 1), shift(down[..., cut:], axis, -1)], -1)
    yield half, far


def solution(mesh):
    finer = Mesh(mesh.devices.reshape(8, 4, 2, 4), AXES)
    placed = (P(DP, None), P(DP, "mp"), P(DP, "mp"), P(DP, "mp"))
    return jax.shard_map(
        shards,
        mesh=finer,
        in_specs=placed,
        out_specs=(P(AXES, None), P(AXES, None), P(None, "mp")),
        check_vma=False,
    )
```
